32 devices in a mesh: cfg: 2 (over y), gx: 8 (over z, x), gy: 2 (over core).
Axes of the slice: x: 2, y: 2, z: 4, core: 2. Of those that a mesh axis runs over, the one named last changes fastest.
Arguments:
- gauge_links: float32 [4, 12, 16, 16, 1024], P(None, None, ('cfg', 'gx'), 'gy'), parts along dimension 2, may hold values from -1 to 1, as said below
- momentum: float32 [8, 16, 16, 1024], P(None, ('cfg', 'gx'), 'gy'), parts along dimension 1, may hold values from -6 to 6
Outputs:
- new_momentum: float32 [8, 16, 16, 1024], P(None, ('cfg', 'gx'), 'gy'), parts along dimension 1
- new_link: float32 [12, 16, 16, 1024], P(None, ('cfg', 'gx'), 'gy'), parts along dimension 1
The draws below stay inside these ranges and needn't reach their ends.
There are 2 independent parts, one for each index of `cfg`. The reference program is written for one: setup_inputs(seed, part) draws one part's arguments, and reference() takes and returns one part's arrays. A program takes and returns all parts, laid end to end along the dimension named above; each array names one. Nothing has to cross between parts.
Inputs may be any that keep to these rules, and one draw needn't show every extreme that they name: `gauge_links`: for every direction and site the two rows are orthonormal complex 3-vectors up to rounding.
All inputs are finite; a program needn't handle non-finite values.
Results may differ from the reference program's by a relative error of at most 0.0003.
Values sent between devices are 32-bit elements; how exact they have to be, the bound alone decides.
A program may use at most 128 MiB of HBM per device.

```python
import math
import jax
import jax.numpy as jnp
from jax import lax

NZ = 32
NT = 32
NX = 8
NY = 16
ZT = 1024


def draw_gauge_links(key, part):
    shape_site = (4, NX, NY, NZ * NT)
    angles = jax.random.uniform(jax.random.fold_in(key, 21), (8,) + shape_site, jnp.float32)
    angles = 2.0 * math.pi * angles
    angle_a = angles[0]
    angle_b = angles[1]
    angle_c = angles[2]
    phase_one = angles[3]
    phase_two = angles[4]
    phase_three = angles[5]
    phase_q = angles[6]
    phase_r = angles[7]
    first_mag = jnp.stack([jnp.cos(angle_a), jnp.sin(angle_a) * jnp.cos(angle_b), jnp.sin(angle_a) * jnp.sin(angle_b)])
    other_mag = jnp.stack([-jnp.sin(angle_a), jnp.cos(angle_a) * jnp.cos(angle_b), jnp.cos(angle_a) * jnp.sin(angle_b)])
    third_mag = jnp.stack([jnp.zeros_like(angle_b), -jnp.sin(angle_b), jnp.cos(angle_b)])
    phases = jnp.stack([phase_one, phase_two, phase_three])
    first_re = first_mag * jnp.cos(phases)
    first_im = first_mag * jnp.sin(phases)
    other_re = other_mag * jnp.cos(phases + phase_q[None])
    other_im = other_mag * jnp.sin(phases + phase_q[None])
    third_re = third_mag * jnp.cos(phases + phase_r[None])
    third_im = third_mag * jnp.sin(phases + phase_r[None])
    weight_one = jnp.cos(angle_c)[None]
    weight_two = jnp.sin(angle_c)[None]
    second_re = weight_one * other_re + weight_two * third_re
    second_im = weight_one * other_im + weight_two * third_im
    rows_re = jnp.stack([first_re, second_re], axis=1)
    rows_im = jnp.stack([first_im, second_im], axis=1)
    rows_re = jnp.moveaxis(rows_re, 0, 2)
    rows_im = jnp.moveaxis(rows_im, 0, 2)
    return jnp.concatenate([rows_re.reshape((4, 6, NX, NY, NZ * NT)), rows_im.reshape((4, 6, NX, NY, NZ * NT))], axis=1)


def level_of(own_key, extent, pieces, low, largest):
    def one(position, shards_of):
        draws = jax.random.uniform(jax.random.fold_in(jax.random.fold_in(own_key, 6), position), (shards_of,), jnp.float32, low / len(pieces), largest / len(pieces))
        return jnp.repeat(jnp.exp(draws), extent[position] // shards_of).reshape((-1,) + (1,) * (len(extent) - position - 1))

    gain = one(*pieces[0])
    for cut in pieces[1:]:
        gain = gain * one(*cut)
    return gain


def scatter_about(stream_key, shape, spread, most, shards=(), kind=jnp.bfloat16):
    array = spread * jax.random.normal(stream_key, shape, jnp.float32)
    if shards:
        array = array * level_of(stream_key, shape, shards, -0.22, 0.18)
    return jnp.clip(array, -most, most).astype(kind)


def setup_inputs(seed: int = 0, part: int = 0) -> dict:
    seeds = jax.random.split(jax.random.key(seed), 3)
    part_splits = jax.random.split(jax.random.fold_in(seeds[2], part), 3)
    gauge_links = draw_gauge_links(jax.random.fold_in(jax.random.fold_in(seeds[2], part), 71), part)
    momentum = scatter_about(part_splits[1], (8, NX, NY, ZT), 1.0, 6.0, ((1, 8), (2, 2)), jnp.float32)
    return dict(gauge_links=gauge_links, momentum=momentum)


coupling = 6.0
step_force = 0.3
step_link = 0.15
kernel_mass = 0.01

def entry_prod(left_mat, right_mat):
    return lax.optimization_barrier(jnp.sum(left_mat[:, :, None] * right_mat[None, :, :], axis=1))

def su3_product(left_pair, right_pair):
    return (entry_prod(left_pair[0], right_pair[0]) - entry_prod(left_pair[1], right_pair[1]), entry_prod(left_pair[0], right_pair[1]) + entry_prod(left_pair[1], right_pair[0]))

def adjoint(matrix):
    return (jnp.swapaxes(matrix[0], 0, 1), -jnp.swapaxes(matrix[1], 0, 1))

def unpack(packed):
    rest = packed.shape[1:]
    rows_re = packed[0:6].reshape((2, 3) + rest)
    rows_im = packed[6:12].reshape((2, 3) + rest)
    third_re = []
    third_im = []
    for column in range(3):
        first_col = (column + 1) % 3
        second_col = (column + 2) % 3
        cross_re = rows_re[0, first_col] * rows_re[1, second_col] - rows_im[0, first_col] * rows_im[1, second_col] - (rows_re[0, second_col] * rows_re[1, first_col] - rows_im[0, second_col] * rows_im[1, first_col])
        cross_im = rows_re[0, first_col] * rows_im[1, second_col] + rows_im[0, first_col] * rows_re[1, second_col] - (rows_re[0, second_col] * rows_im[1, first_col] + rows_im[0, second_col] * rows_re[1, first_col])
        third_re.append(cross_re)
        third_im.append(-cross_im)
    return (jnp.concatenate([rows_re, jnp.stack(third_re)[None]], axis=0), jnp.concatenate([rows_im, jnp.stack(third_im)[None]], axis=0))

def algebra_parts(matrix):
    whole_re, whole_im = matrix
    root_three = math.sqrt(3.0)
    parts_list = [whole_im[1, 0] + whole_im[0, 1], whole_re[0, 1] - whole_re[1, 0], whole_im[0, 0] - whole_im[1, 1], whole_im[2, 0] + whole_im[0, 2], whole_re[0, 2] - whole_re[2, 0], whole_im[2, 1] + whole_im[1, 2], whole_re[1, 2] - whole_re[2, 1], (whole_im[0, 0] + whole_im[1, 1] - 2.0 * whole_im[2, 2]) / root_three]
    return jnp.stack(parts_list)

def algebra_matrix(parts):
    root_inv = 1.0 / math.sqrt(3.0)
    zero_part = jnp.zeros_like(parts[0])
    herm_re = jnp.stack([jnp.stack([0.5 * (parts[2] + root_inv * parts[7]), 0.5 * parts[0], 0.5 * parts[3]]), jnp.stack([0.5 * parts[0], 0.5 * (root_inv * parts[7] - parts[2]), 0.5 * parts[5]]), jnp.stack([0.5 * parts[3], 0.5 * parts[5], -root_inv * parts[7]])])
    herm_im = jnp.stack([jnp.stack([zero_part, -0.5 * parts[1], -0.5 * parts[4]]), jnp.stack([0.5 * parts[1], zero_part, -0.5 * parts[6]]), jnp.stack([0.5 * parts[4], 0.5 * parts[6], zero_part])])
    return (herm_re, herm_im)

def link_exp(parts):
    herm_re, herm_im = algebra_matrix(parts)
    gen_re = -0.25 * step_link * herm_im
    gen_im = 0.25 * step_link * herm_re
    eye_mat = jnp.eye(3, dtype=jnp.float32)[:, :, None, None, None] + jnp.zeros_like(gen_re)
    series = (eye_mat, jnp.zeros_like(gen_re))
    for series_order in range(6, 0, -1):
        grown = su3_product((gen_re, gen_im), series)
        series = (eye_mat + grown[0] / series_order, grown[1] / series_order)
    for square_step in range(2):
        series = su3_product(series, series)
    return series

def move_field(field_data, lattice_dim, offset):
    if lattice_dim < 2:
        return jnp.roll(field_data, -offset, axis=2 + lattice_dim)
    leading = field_data.shape[:-1]
    lattice = field_data.reshape(leading + (NZ, NT))
    lattice = jnp.roll(lattice, -offset, axis=len(leading) + lattice_dim - 2)
    return lattice.reshape(field_data.shape)

def moved(matrix, lattice_dim, offset):
    return (move_field(matrix[0], lattice_dim, offset), move_field(matrix[1], lattice_dim, offset))

def sine_squares(length):
    phase_angle = jnp.arange(length, dtype=jnp.int32).astype(jnp.float32) * (math.pi / length)
    return jnp.sin(phase_angle) * jnp.sin(phase_angle)

def reference(gauge_links, momentum):
    link_x = unpack(gauge_links[0])
    staple_re = jnp.zeros_like(link_x[0])
    staple_im = jnp.zeros_like(link_x[0])
    for direction in range(1, 4):
        link_nu = unpack(gauge_links[direction])
        ahead_nu = moved(link_nu, 0, 1)
        upper_staple = su3_product(su3_product(ahead_nu, adjoint(moved(link_x, direction, 1))), adjoint(link_nu))
        lower_staple = su3_product(su3_product(adjoint(moved(ahead_nu, direction, -1)), adjoint(moved(link_x, direction, -1))), moved(link_nu, direction, -1))
        staple_re = staple_re + upper_staple[0] + lower_staple[0]
        staple_im = staple_im + upper_staple[1] + lower_staple[1]
    loop_sum = su3_product(link_x, (staple_re, staple_im))
    force_parts = coupling / 6.0 * algebra_parts(loop_sum)
    new_momentum = momentum - step_force * force_parts
    lattice = new_momentum.reshape((8, NX, NY, NZ, NT))
    spectrum = jnp.fft.fftn(lattice, axes=(1, 2, 3, 4))
    plane_part = sine_squares(NZ)[:, None] + sine_squares(NT)[None, :]
    denom = kernel_mass + 4.0 * (sine_squares(NX)[:, None, None, None] + sine_squares(NY)[None, :, None, None] + plane_part[None, None, :, :])
    kernel_values = 4.0 / denom
    smooth = jnp.real(jnp.fft.ifftn(spectrum * kernel_values[None], axes=(1, 2, 3, 4))).astype(jnp.float32)
    smooth = smooth.reshape(new_momentum.shape)
    rotation = link_exp(smooth)
    updated = su3_product(rotation, link_x)
    rest = new_momentum.shape[1:]
    new_link = jnp.concatenate([updated[0][0:2].reshape((6,) + rest), updated[1][0:2].reshape((6,) + rest)], axis=0)
    return (new_momentum, new_link)
```

```python
import math

import jax
import jax.numpy as jnp
import numpy as np
from jax import lax
from jax.experimental import pallas as pl
from jax.experimental.pallas import tpu as pltpu
from jax.sharding import PartitionSpec as P

NZ = 32
NT = 32

coupling = 6.0
step_force = 0.3
step_link = 0.15
kernel_mass = 0.01

LANES = 128


def hartley(length):
    index = np.arange(length)
    angle = (index[:, None] * index[None, :] % length) * (2.0 * math.pi / length)
    return (np.cos(angle) + np.sin(angle)) / math.sqrt(length)


def sine_squares(length):
    return np.sin(np.arange(length) * (math.pi / length)) ** 2


def tables(x_total, y_total, count, parts):
    mix_xy = np.kron(hartley(x_total), hartley(y_total)).astype(np.float32)
    row_part = 4.0 * (sine_squares(x_total)[:, None] + sine_squares(y_total)[None, :])
    row_part = (kernel_mass + row_part).reshape(-1, 1).astype(np.float32)
    plane = 4.0 * (sine_squares(NZ)[:, None] + sine_squares(NT)[None, :]).reshape(-1)
    plane = np.tile(plane, count).reshape(parts, 1, -1).astype(np.float32)
    z_rows = np.repeat(hartley(NZ), NT, axis=1).reshape(NZ, 1, NZ * NT).astype(np.float32)
    t_rows = np.tile(hartley(NT), (1, NZ)).astype(np.float32)
    return mix_xy, row_part, plane, z_rows, t_rows


def cmul_sum(terms):
    real, imag = None, None
    for (a, b), (c, d) in terms:
        re = a * c - b * d
        im = a * d + b * c
        real = re if real is None else real + re
        imag = im if imag is None else imag + im
    return (real, imag)


def product(left, right):
    return [
        [cmul_sum([(left[i][m], right[m][k]) for m in range(3)]) for k in range(len(right[0]))]
        for i in range(len(left))
    ]


def adjoint(matrix):
    return [[(matrix[k][i][0], -matrix[k][i][1]) for k in range(3)] for i in range(3)]


def third_row(rows):
    third = []
    for column in range(3):
        j, k = (column + 1) % 3, (column + 2) % 3
        (ar, ai), (br, bi) = rows[0][j], rows[1][k]
        (cr, ci), (dr, di) = rows[0][k], rows[1][j]
        third.append((ar * br - ai * bi - (cr * dr - ci * di), -(ar * bi + ai * br - (cr * di + ci * dr))))
    return [rows[0], rows[1], third]


def load_link(ref, lanes):
    rows = [[(ref[3 * r + k, :, lanes], ref[6 + 3 * r + k, :, lanes]) for k in range(3)] for r in range(2)]
    return third_row(rows)


def algebra_parts(left, right):
    full = product(left, right)

    def re(i, k):
        return full[i][k][0]

    def im(i, k):
        return full[i][k][1]

    return [
        im(1, 0) + im(0, 1),
        re(0, 1) - re(1, 0),
        im(0, 0) - im(1, 1),
        im(2, 0) + im(0, 2),
        re(0, 2) - re(2, 0),
        im(2, 1) + im(1, 2),
        re(1, 2) - re(2, 1),
        (im(0, 0) + im(1, 1) - 2.0 * im(2, 2)) * (1.0 / math.sqrt(3.0)),
    ]


def square(c, p, q):
    c0, c1, c2 = c

    def mul(a, b):
        return (a[0] * b[0] - a[1] * b[1], a[0] * b[1] + a[1] * b[0])

    def sq(a):
        return (a[0] * a[0] - a[1] * a[1], 2.0 * (a[0] * a[1]))

    c01, c02, c12 = mul(c0, c1), mul(c0, c2), mul(c1, c2)
    s0, s1, s2 = sq(c0), sq(c1), sq(c2)
    return [
        tuple(s0[i] + 2.0 * (c12[i] * q) for i in range(2)),
        tuple(2.0 * (c01[i] + c12[i] * p) + s2[i] * q for i in range(2)),
        tuple(s1[i] + 2.0 * c02[i] + s2[i] * p for i in range(2)),
    ]


def rotation_rows(parts):
    scale = 0.25 * step_link
    root_inv = 1.0 / math.sqrt(3.0)
    g = [0.5 * scale * part for part in parts]
    g8 = root_inv * g[7]
    b00, b11, b22 = g8 + g[2], g8 - g[2], -2.0 * g8
    b01, b02, b12 = (g[0], -g[1]), (g[3], -g[4]), (g[5], -g[6])

    def norm(a):
        return a[0] * a[0] + a[1] * a[1]

    n01, n02, n12 = norm(b01), norm(b02), norm(b12)
    d00, d11 = b00 * b00 + n01 + n02, b11 * b11 + n01 + n12
    p = 0.5 * (b00 * b00 + b11 * b11 + b22 * b22) + n01 + n02 + n12
    t_re = b01[0] * b12[0] - b01[1] * b12[1]
    t_im = b01[0] * b12[1] + b01[1] * b12[0]
    q = b00 * b11 * b22 + 2.0 * (t_re * b02[0] + t_im * b02[1]) - b00 * n12 - b11 * n02 - b22 * n01
    e01 = (b01[0] * (b00 + b11) + b02[0] * b12[0] + b02[1] * b12[1],
           b01[1] * (b00 + b11) + b02[1] * b12[0] - b02[0] * b12[1])
    e02 = (b02[0] * (b00 + b22) + t_re, b02[1] * (b00 + b22) + t_im)
    e12 = (b12[0] * (b11 + b22) + b01[0] * b02[0] + b01[1] * b02[1],
           b12[1] * (b11 + b22) + b01[0] * b02[1] - b01[1] * b02[0])
    p2, pq = p * p, p * q
    c = [
        (1.0 - q * q * (1.0 / 720), pq * (1.0 / 120) - q * (1.0 / 6)),
        (q * (1.0 / 24) - pq * (1.0 / 360), 1.0 - p * (1.0 / 6) + p2 * (1.0 / 120)),
        (p * (1.0 / 24) - 0.5 - p2 * (1.0 / 720), q * (1.0 / 120)),
    ]
    c = square(square(c, p, q), p, q)
    c0, c1, c2 = c

    def diag(b, d):
        return tuple(c0[i] + c1[i] * b + c2[i] * d for i in range(2))

    def off(b, d, sign):
        bi, di = (b[1], d[1]) if sign > 0 else (-b[1], -d[1])
        return (
            c1[0] * b[0] - c1[1] * bi + c2[0] * d[0] - c2[1] * di,
            c1[0] * bi + c1[1] * b[0] + c2[0] * di + c2[1] * d[0],
        )

    return [
        [diag(b00, d00), off(b01, e01, 1), off(b02, e02, 1)],
        [off(b01, e01, -1), diag(b11, d11), off(b12, e12, 1)],
    ]


def split(value):
    high = value.astype(jnp.bfloat16)
    return high, (value - high.astype(jnp.float32)).astype(jnp.bfloat16)


def plane_transform(value, high_ref, low_ref):
    rows = value.shape[0]
    high, low = split(value)
    both = jnp.dot(jnp.concatenate([high, low], axis=0), high_ref[...], preferred_element_type=jnp.float32)
    rest = jnp.dot(high, low_ref[...], preferred_element_type=jnp.float32)
    return both[:rows] + both[rows:] + rest


def move_z(value, steps):
    return pltpu.roll(value, (steps * NT) % value.shape[1], 1)


def move_t(value, steps):
    lanes = value.shape[1]
    inside = pltpu.roll(value, steps % lanes, 1)
    beside = pltpu.roll(value, (steps - steps * NT) % lanes, 1)
    t_index = lax.broadcasted_iota(jnp.int32, value.shape, 1) % NT
    wraps = jnp.logical_or(t_index - steps < 0, t_index - steps >= NT)
    return jnp.where(wraps, beside, inside)


def move_y(value, beyond, steps):
    rows = value.shape[0]
    row_index = lax.broadcasted_iota(jnp.int32, value.shape, 0)
    edge = row_index == (0 if steps > 0 else rows - 1)
    shift = steps % rows
    return jnp.where(edge, pltpu.roll(beyond, shift, 0), pltpu.roll(value, shift, 0))


def step_kernel(
    gx_count, gy_count,
    links, momentum, mix_xy, row_part, plane, z_rows, t_rows,
    out_momentum, out_link,
    ahead, peer_x, shifted_x, lower, peer_lower, total,
    outgoing, gathered, filtered, returned, table_high, table_low, weights,
    halo_send, halo_recv, peer_send, peer_recv, out_send, out_recv, back_send, back_recv,
):
    gx, gy = lax.axis_index("gx"), lax.axis_index("gy")
    parts = gx_count * gy_count
    me = gx * gy_count + gy
    colors, rows, sites = momentum.shape
    width = outgoing.shape[2]
    chunks = sites // LANES
    behind = {"gx": lax.rem(gx + gx_count - 1, gx_count), "gy": gy}
    y_after = {"gx": gx, "gy": lax.rem(gy + 1, gy_count)}
    y_before = {"gx": gx, "gy": lax.rem(gy + gy_count - 1, gy_count)}

    def place(index):
        return {"gx": index // gy_count, "gy": lax.rem(index, gy_count)}

    barrier = pltpu.get_barrier_semaphore()

    def greet(offset, carry):
        pl.semaphore_signal(barrier, inc=1, device_id=place(lax.rem(me + offset, parts)))
        return carry

    lax.fori_loop(1, parts, greet, 0)
    pl.semaphore_wait(barrier, parts - 1)

    halo = [
        pltpu.make_async_remote_copy(
            links.at[nu + 1], ahead.at[nu], halo_send.at[nu], halo_recv.at[nu], device_id=behind
        )
        for nu in range(3)
    ]
    fetch_x = pltpu.make_async_remote_copy(
        links.at[0], peer_x, peer_send.at[0], peer_recv.at[0], device_id=y_before
    )
    fetch_x.start()
    for copy in halo:
        copy.start()

    def make_table(z, carry):
        block = t_rows[...] * z_rows[z]
        high, low = split(block)
        at = pl.ds(pl.multiple_of(z * NT, NT), NT)
        table_high[at, :] = high
        table_low[at, :] = low
        return carry

    lax.fori_loop(0, NZ, make_table, 0)
    weights[...] = 4.0 / (row_part[...] + plane[me])

    def shift_sides(entry, carry):
        value = links[0, entry]
        shifted_x[1, entry] = move_z(value, -1)
        shifted_x[2, entry] = move_t(value, -1)
        return carry

    lax.fori_loop(0, 12, shift_sides, 0)
    fetch_x.wait()

    def shift_y(entry, carry):
        shifted_x[0, entry] = move_y(links[0, entry], peer_x[entry], -1)
        return carry

    lax.fori_loop(0, 12, shift_y, 0)

    def direction(nu, first):
        def chunk(j, carry):
            lanes = pl.ds(pl.multiple_of(j * LANES, LANES), LANES)
            link_nu = load_link(links.at[nu + 1], lanes)
            across = load_link(shifted_x.at[nu], lanes)
            corner = product(load_link(links.at[0], lanes), load_link(ahead.at[nu], lanes))
            upper = algebra_parts(corner, adjoint(product(link_nu, across)))
            below = algebra_parts(product(across, adjoint(corner)), link_nu)
            for a in range(8):
                total[a, :, lanes] = upper[a] if first else total[a, :, lanes] + upper[a]
                lower[nu, a, :, lanes] = below[a]
            return carry

        lax.fori_loop(0, chunks, chunk, 0)

    halo[0].wait()
    direction(0, True)
    send_lower = pltpu.make_async_remote_copy(
        lower.at[0], peer_lower, peer_send.at[1], peer_recv.at[1], device_id=y_after
    )
    send_lower.start()
    halo[1].wait()
    direction(1, False)
    send_lower.wait()
    halo[2].wait()
    direction(2, False)

    def finish(a, carry):
        force = total[a] + move_z(lower[1, a], 1) + move_t(lower[2, a], 1)
        force = force + move_y(lower[0, a], peer_lower[a], 1)
        out_momentum[a] = momentum[a] - (step_force * coupling / 6.0) * force
        return carry

    lax.fori_loop(0, 8, finish, 0)

    spectrum = plane_transform(out_momentum[...].reshape(colors * rows, sites), table_high, table_low)
    spectrum = spectrum.reshape(colors, rows, sites)
    pieces = sites // width
    for part in range(parts):
        c, k = part // pieces, part % pieces
        outgoing[part] = spectrum[c, :, k * width : (k + 1) * width]

    def own_rows(index):
        return pl.ds(pl.multiple_of(index * rows, rows), rows)

    def out_copy(to, source):
        return pltpu.make_async_remote_copy(
            outgoing.at[to], gathered.at[own_rows(source)], out_send.at[to], out_recv.at[source],
            device_id=place(to),
        )

    def start_out(offset, carry):
        out_copy(lax.rem(me + offset, parts), me).start()
        return carry

    def wait_out(offset, carry):
        other = lax.rem(me + offset, parts)
        out_copy(other, other).wait()
        return carry

    lax.fori_loop(1, parts, start_out, 0)
    gathered[own_rows(me), :] = outgoing[me]
    lax.fori_loop(1, parts, wait_out, 0)

    def mix(source, target, weighted):
        total_rows = mix_xy.shape[0]
        size = min(total_rows, LANES)

        def block(index, carry):
            at = pl.ds(pl.multiple_of(index * size, size), size)
            mixed = jnp.dot(
                mix_xy[at, :], source[...], preferred_element_type=jnp.float32,
                precision=lax.Precision.HIGHEST,
            )
            target[at, :] = mixed * weights[at, :] if weighted else mixed
            return carry

        lax.fori_loop(0, total_rows // size, block, 0)

    mix(gathered, filtered, True)
    mix(filtered, gathered, False)

    def back_copy(to, source):
        return pltpu.make_async_remote_copy(
            gathered.at[own_rows(to)], returned.at[source], back_send.at[to], back_recv.at[source],
            device_id=place(to),
        )

    def start_back(offset, carry):
        back_copy(lax.rem(me + offset, parts), me).start()
        return carry

    def wait_back(offset, carry):
        other = lax.rem(me + offset, parts)
        back_copy(other, other).wait()
        return carry

    lax.fori_loop(1, parts, start_back, 0)
    returned[me] = gathered[own_rows(me), :]
    lax.fori_loop(1, parts, wait_back, 0)

    back = jnp.concatenate(
        [
            jnp.concatenate([returned[c * pieces + k] for k in range(pieces)], axis=1)
            for c in range(colors)
        ],
        axis=0,
    )
    total[...] = plane_transform(back, table_high, table_low).reshape(colors, rows, sites)

    def update(j, carry):
        lanes = pl.ds(pl.multiple_of(j * LANES, LANES), LANES)
        rotation = rotation_rows([total[a, :, lanes] for a in range(8)])
        updated = product(rotation, load_link(links.at[0], lanes))
        for r in range(2):
            for k in range(3):
                out_link[3 * r + k, :, lanes] = updated[r][k][0]
                out_link[6 + 3 * r + k, :, lanes] = updated[r][k][1]
        return carry

    lax.fori_loop(0, chunks, update, 0)


def shards(gauge_links, momentum):
    gx_count, gy_count = lax.axis_size("gx"), lax.axis_size("gy")
    colors, layers, rows, sites = momentum.shape
    assert layers == 1
    parts = gx_count * gy_count
    width = colors * sites // parts
    assert sites % width == 0
    links = gauge_links.reshape(4, 12, rows, sites)
    fields = momentum.reshape(colors, rows, sites)
    f32 = jnp.float32
    everything = rows * parts
    dma = pltpu.SemaphoreType.DMA

    def body(*refs):
        step_kernel(gx_count, gy_count, *refs)

    vmem = pl.BlockSpec(memory_space=pltpu.VMEM)
    new_momentum, new_link = pl.pallas_call(
        body,
        out_shape=(
            jax.ShapeDtypeStruct((colors, rows, sites), f32),
            jax.ShapeDtypeStruct((12, rows, sites), f32),
        ),
        in_specs=[vmem] * 7,
        out_specs=(vmem, vmem),
        scratch_shapes=[
            pltpu.VMEM((3, 12, rows, sites), f32),
            pltpu.VMEM((12, rows, sites), f32),
            pltpu.VMEM((3, 12, rows, sites), f32),
            pltpu.VMEM((3, colors, rows, sites), f32),
            pltpu.VMEM((colors, rows, sites), f32),
            pltpu.VMEM((colors, rows, sites), f32),
            pltpu.VMEM((parts, rows, width), f32),
            pltpu.VMEM((everything, width), f32),
            pltpu.VMEM((everything, width), f32),
            pltpu.VMEM((parts, rows, width), f32),
            pltpu.VMEM((sites, sites), jnp.bfloat16),
            pltpu.VMEM((sites, sites), jnp.bfloat16),
            pltpu.VMEM((everything, width), f32),
            dma((3,)), dma((3,)), dma((2,)), dma((2,)),
            dma((parts,)), dma((parts,)), dma((parts,)), dma((parts,)),
        ],
        compiler_params=pltpu.CompilerParams(
            collective_id=0, has_side_effects=True, vmem_limit_bytes=60 * 1024 * 1024
        ),
    )(links, fields, *tables(gx_count * layers, gy_count * rows, colors, parts))
    return (new_momentum.reshape(momentum.shape), new_link.reshape((12,) + momentum.shape[1:]))


def solution(mesh):
    return jax.shard_map(
        shards,
        mesh=mesh,
        in_specs=(P(None, None, ("cfg", "gx"), "gy", None), P(None, ("cfg", "gx"), "gy", None)),
        out_specs=(P(None, ("cfg", "gx"), "gy", None), P(None, ("cfg", "gx"), "gy", None)),
        check_vma=False,
    )
```

```python
import math

import jax
import jax.numpy as jnp
import numpy as np
from jax import lax
from jax.experimental import pallas as pl
from jax.experimental.pallas import tpu as pltpu
from jax.sharding import PartitionSpec as P

NZ = 32
NT = 32

coupling = 6.0
step_force = 0.3
step_link = 0.15
kernel_mass = 0.01

LANES = 128
HALVES = 2


def hartley(length):
    index = np.arange(length)
    angle = (index[:, None] * index[None, :] % length) * (2.0 * math.pi / length)
    return (np.cos(angle) + np.sin(angle)) / math.sqrt(length)


def sine_squares(length):
    return np.sin(np.arange(length) * (math.pi / length)) ** 2


def tables(x_total, y_total, count, parts):
    mix_xy = np.kron(hartley(x_total), hartley(y_total)).astype(np.float32)
    row_part = 4.0 * (sine_squares(x_total)[:, None] + sine_squares(y_total)[None, :])
    row_part = (kernel_mass + row_part).reshape(-1, 1).astype(np.float32)
    plane = 4.0 * (sine_squares(NZ)[:, None] + sine_squares(NT)[None, :]).reshape(-1)
    plane = np.tile(plane, count).reshape(parts, 1, -1).astype(np.float32)
    z_rows = np.repeat(hartley(NZ), NT, axis=1).reshape(NZ, 1, NZ * NT).astype(np.float32)
    t_rows = np.tile(hartley(NT), (1, NZ)).astype(np.float32)
    return mix_xy, row_part, plane, z_rows, t_rows


def cmul_sum(terms):
    real, imag = None, None
    for (a, b), (c, d) in terms:
        re = a * c - b * d
        im = a * d + b * c
        real = re if real is None else real + re
        imag = im if imag is None else imag + im
    return (real, imag)


def product(left, right):
    return [
        [cmul_sum([(left[i][m], right[m][k]) for m in range(3)]) for k in range(len(right[0]))]
        for i in range(len(left))
    ]


def adjoint(matrix):
    return [[(matrix[k][i][0], -matrix[k][i][1]) for k in range(3)] for i in range(3)]


def third_row(rows):
    third = []
    for column in range(3):
        j, k = (column + 1) % 3, (column + 2) % 3
        (ar, ai), (br, bi) = rows[0][j], rows[1][k]
        (cr, ci), (dr, di) = rows[0][k], rows[1][j]
        third.append((ar * br - ai * bi - (cr * dr - ci * di), -(ar * bi + ai * br - (cr * di + ci * dr))))
    return [rows[0], rows[1], third]


def load_link(ref, lanes):
    rows = [[(ref[3 * r + k, :, lanes], ref[6 + 3 * r + k, :, lanes]) for k in range(3)] for r in range(2)]
    return third_row(rows)


def stereographic(pole, others):
    size = sum(x * x for x in others[1:]) + others[0] * others[0]
    south = pole < 0.0
    factor = jnp.where(south, 1.0 - pole, 1.0) / jnp.where(south, jnp.maximum(size, 1e-24), 1.0 + pole)
    out = [x * factor for x in others]
    out[0] = jnp.where(jnp.logical_and(south, size < 1e-24), 1e12, out[0])
    return out


def encode(rows):
    out = []
    for row in rows:
        out += stereographic(row[0][0], [row[0][1], row[1][0], row[1][1], row[2][0], row[2][1]])
    return out


def decode(values):
    rows = []
    for y in (values[:5], values[5:]):
        n = sum(x * x for x in y[1:]) + y[0] * y[0]
        near = 1.0 / (1.0 + n)
        twice = 2.0 * near
        u = [x * twice for x in y]
        rows.append([((1.0 - n) * near, u[0]), (u[1], u[2]), (u[3], u[4])])
    return third_row(rows)


def algebra_parts(left, right):
    full = product(left, right)

    def re(i, k):
        return full[i][k][0]

    def im(i, k):
        return full[i][k][1]

    return [
        im(1, 0) + im(0, 1),
        re(0, 1) - re(1, 0),
        im(0, 0) - im(1, 1),
        im(2, 0) + im(0, 2),
        re(0, 2) - re(2, 0),
        im(2, 1) + im(1, 2),
        re(1, 2) - re(2, 1),
        (im(0, 0) + im(1, 1) - 2.0 * im(2, 2)) * (1.0 / math.sqrt(3.0)),
    ]


def square(c, p, q):
    c0, c1, c2 = c

    def mul(a, b):
        return (a[0] * b[0] - a[1] * b[1], a[0] * b[1] + a[1] * b[0])

    def sq(a):
        return (a[0] * a[0] - a[1] * a[1], 2.0 * (a[0] * a[1]))

    c01, c02, c12 = mul(c0, c1), mul(c0, c2), mul(c1, c2)
    s0, s1, s2 = sq(c0), sq(c1), sq(c2)
    return [
        tuple(s0[i] + 2.0 * (c12[i] * q) for i in range(2)),
        tuple(2.0 * (c01[i] + c12[i] * p) + s2[i] * q for i in range(2)),
        tuple(s1[i] + 2.0 * c02[i] + s2[i] * p for i in range(2)),
    ]


def rotation_rows(parts):
    scale = 0.25 * step_link
    root_inv = 1.0 / math.sqrt(3.0)
    g = [0.5 * scale * part for part in parts]
    g8 = root_inv * g[7]
    b00, b11, b22 = g8 + g[2], g8 - g[2], -2.0 * g8
    b01, b02, b12 = (g[0], -g[1]), (g[3], -g[4]), (g[5], -g[6])

    def norm(a):
        return a[0] * a[0] + a[1] * a[1]

    n01, n02, n12 = norm(b01), norm(b02), norm(b12)
    d00, d11 = b00 * b00 + n01 + n02, b11 * b11 + n01 + n12
    p = 0.5 * (b00 * b00 + b11 * b11 + b22 * b22) + n01 + n02 + n12
    t_re = b01[0] * b12[0] - b01[1] * b12[1]
    t_im = b01[0] * b12[1] + b01[1] * b12[0]
    q = b00 * b11 * b22 + 2.0 * (t_re * b02[0] + t_im * b02[1]) - b00 * n12 - b11 * n02 - b22 * n01
    e01 = (b01[0] * (b00 + b11) + b02[0] * b12[0] + b02[1] * b12[1],
           b01[1] * (b00 + b11) + b02[1] * b12[0] - b02[0] * b12[1])
    e02 = (b02[0] * (b00 + b22) + t_re, b02[1] * (b00 + b22) + t_im)
    e12 = (b12[0] * (b11 + b22) + b01[0] * b02[0] + b01[1] * b02[1],
           b12[1] * (b11 + b22) + b01[0] * b02[1] - b01[1] * b02[0])
    p2, pq = p * p, p * q
    c = [
        (1.0 - q * q * (1.0 / 720), pq * (1.0 / 120) - q * (1.0 / 6)),
        (q * (1.0 / 24) - pq * (1.0 / 360), 1.0 - p * (1.0 / 6) + p2 * (1.0 / 120)),
        (p * (1.0 / 24) - 0.5 - p2 * (1.0 / 720), q * (1.0 / 120)),
    ]
    c = square(square(c, p, q), p, q)
    c0, c1, c2 = c

    def diag(b, d):
        return tuple(c0[i] + c1[i] * b + c2[i] * d for i in range(2))

    def off(b, d, sign):
        bi, di = (b[1], d[1]) if sign > 0 else (-b[1], -d[1])
        return (
            c1[0] * b[0] - c1[1] * bi + c2[0] * d[0] - c2[1] * di,
            c1[0] * bi + c1[1] * b[0] + c2[0] * di + c2[1] * d[0],
        )

    return [
        [diag(b00, d00), off(b01, e01, 1), off(b02, e02, 1)],
        [off(b01, e01, -1), diag(b11, d11), off(b12, e12, 1)],
    ]


def split(value):
    high = value.astype(jnp.bfloat16)
    return high, (value - high.astype(jnp.float32)).astype(jnp.bfloat16)


def plane_transform(value, high_ref, low_ref):
    rows = value.shape[0]
    high, low = split(value)
    both = jnp.dot(jnp.concatenate([high, low], axis=0), high_ref[...], preferred_element_type=jnp.float32)
    rest = jnp.dot(high, low_ref[...], preferred_element_type=jnp.float32)
    return both[:rows] + both[rows:] + rest


def move_z(value, steps):
    return pltpu.roll(value, (steps * NT) % value.shape[1], 1)


def move_t(value, steps):
    lanes = value.shape[1]
    inside = pltpu.roll(value, steps % lanes, 1)
    beside = pltpu.roll(value, (steps - steps * NT) % lanes, 1)
    t_index = lax.broadcasted_iota(jnp.int32, value.shape, 1) % NT
    wraps = jnp.logical_or(t_index - steps < 0, t_index - steps >= NT)
    return jnp.where(wraps, beside, inside)


def move_y(value, beyond, steps):
    rows = value.shape[0]
    row_index = lax.broadcasted_iota(jnp.int32, value.shape, 0)
    edge = row_index == (0 if steps > 0 else rows - 1)
    shift = steps % rows
    return jnp.where(edge, pltpu.roll(beyond, shift, 0), pltpu.roll(value, shift, 0))


def step_kernel(
    gx_count, gy_count,
    links_far, momentum, mix_xy, row_part, plane, z_rows, t_rows,
    out_momentum, out_link,
    links, crossed, coded, ahead, peer_x, shifted_x, lower, peer_lower, total,
    outgoing, gathered, filtered, returned, table_high, table_low, weights,
    load_sem, halo_send, halo_recv, peer_send, peer_recv, out_send, out_recv, back_send, back_recv,
):
    gx, gy = lax.axis_index("gx"), lax.axis_index("gy")
    parts = gx_count * gy_count
    me = gx * gy_count + gy
    colors, rows, sites = momentum.shape
    width = outgoing.shape[2]
    chunks = sites // LANES
    behind = {"gx": lax.rem(gx + gx_count - 1, gx_count), "gy": gy}
    y_after = {"gx": gx, "gy": lax.rem(gy + 1, gy_count)}
    y_before = {"gx": gx, "gy": lax.rem(gy + gy_count - 1, gy_count)}

    def place(index):
        return {"gx": index // gy_count, "gy": lax.rem(index, gy_count)}

    barrier = pltpu.get_barrier_semaphore()

    def greet(offset, carry):
        pl.semaphore_signal(barrier, inc=1, device_id=place(lax.rem(me + offset, parts)))
        return carry

    lax.fori_loop(1, parts, greet, 0)
    loads = [pltpu.make_async_copy(links_far.at[d], links.at[d], load_sem.at[d]) for d in range(4)]
    for d in (1, 2, 3, 0):
        loads[d].start()

    def pack(nu):
        def chunk(j, carry):
            lanes = pl.ds(pl.multiple_of(j * LANES, LANES), LANES)
            ref = links.at[nu + 1]
            rows_of = [
                [(ref[3 * r + k, :, lanes], ref[6 + 3 * r + k, :, lanes]) for k in range(3)]
                for r in range(2)
            ]
            for index, value in enumerate(encode(rows_of)):
                coded[nu, index, :, lanes] = value
            return carry

        loads[nu + 1].wait()
        lax.fori_loop(0, chunks, chunk, 0)

    half = sites // HALVES

    def halo_copy(nu, piece):
        lanes = pl.ds(piece * half, half)
        slot = nu * HALVES + piece
        return pltpu.make_async_remote_copy(
            coded.at[nu, :, :, lanes], ahead.at[nu, :, :, lanes],
            halo_send.at[slot], halo_recv.at[slot], device_id=behind,
        )

    halo = [[halo_copy(nu, piece) for piece in range(HALVES)] for nu in range(3)]
    fetch_x = pltpu.make_async_remote_copy(
        links_far.at[0], peer_x, peer_send.at[0], peer_recv.at[0], device_id=y_before
    )
    pack(0)
    pl.semaphore_wait(barrier, parts - 1)
    for nu in range(3):
        if nu > 0:
            pack(nu)
        for copy in halo[nu]:
            copy.start()
    fetch_x.start()

    def make_table(z, carry):
        block = t_rows[...] * z_rows[z]
        high, low = split(block)
        at = pl.ds(pl.multiple_of(z * NT, NT), NT)
        table_high[at, :] = high
        table_low[at, :] = low
        return carry

    lax.fori_loop(0, NZ, make_table, 0)
    weights[...] = 4.0 / (row_part[...] + plane[me])

    loads[0].wait()

    def shift_sides(entry, carry):
        value = links[0, entry]
        shifted_x[1, entry] = move_z(value, -1)
        shifted_x[2, entry] = move_t(value, -1)
        return carry

    lax.fori_loop(0, 12, shift_sides, 0)
    fetch_x.wait()

    def shift_y(entry, carry):
        shifted_x[0, entry] = move_y(links[0, entry], peer_x[entry], -1)
        return carry

    lax.fori_loop(0, 12, shift_y, 0)

    def cross(nu):
        def chunk(j, carry):
            lanes = pl.ds(pl.multiple_of(j * LANES, LANES), LANES)
            pair = product(load_link(links.at[nu + 1], lanes), load_link(shifted_x.at[nu], lanes))
            for i in range(3):
                for k in range(3):
                    crossed[nu, 3 * i + k, :, lanes] = pair[i][k][0]
                    crossed[nu, 9 + 3 * i + k, :, lanes] = pair[i][k][1]
            return carry

        lax.fori_loop(0, chunks, chunk, 0)

    for nu in range(3):
        cross(nu)

    def direction(nu, piece):
        per = chunks // HALVES

        def chunk(j, carry):
            lanes = pl.ds(pl.multiple_of(j * LANES, LANES), LANES)
            link_nu = load_link(links.at[nu + 1], lanes)
            across = load_link(shifted_x.at[nu], lanes)
            corner = product(load_link(links.at[0], lanes), decode([ahead[nu, e, :, lanes] for e in range(10)]))
            pair = [
                [
                    (crossed[nu, 3 * i + k, :, lanes], crossed[nu, 9 + 3 * i + k, :, lanes])
                    for k in range(3)
                ]
                for i in range(3)
            ]
            upper = algebra_parts(corner, adjoint(pair))
            below = algebra_parts(product(across, adjoint(corner)), link_nu)
            for a in range(8):
                total[a, :, lanes] = upper[a] if nu == 0 else total[a, :, lanes] + upper[a]
                lower[nu, a, :, lanes] = below[a]
            return carry

        lax.fori_loop(piece * per, (piece + 1) * per, chunk, 0)

    send_lower = pltpu.make_async_remote_copy(
        lower.at[0], peer_lower, peer_send.at[1], peer_recv.at[1], device_id=y_after
    )
    for nu in range(3):
        for piece in range(HALVES):
            halo[nu][piece].wait()
            direction(nu, piece)
        if nu == 0:
            send_lower.start()
        if nu == 1:
            send_lower.wait()

    def finish(a, carry):
        force = total[a] + move_z(lower[1, a], 1) + move_t(lower[2, a], 1)
        force = force + move_y(lower[0, a], peer_lower[a], 1)
        out_momentum[a] = momentum[a] - (step_force * coupling / 6.0) * force
        return carry

    lax.fori_loop(0, 8, finish, 0)

    def own_rows(index):
        return pl.ds(pl.multiple_of(index * rows, rows), rows)

    def out_copy(to, source):
        return pltpu.make_async_remote_copy(
            outgoing.at[to], gathered.at[own_rows(source)], out_send.at[to], out_recv.at[source],
            device_id=place(to),
        )

    pieces = sites // width
    groups = min(2, pieces)
    group_sites = sites // groups
    fields = out_momentum[...].reshape(colors * rows, sites)
    for group in range(groups):
        at = slice(group * group_sites, (group + 1) * group_sites)
        spectrum = plane_transform(fields, table_high.at[:, at], table_low.at[:, at])
        spectrum = spectrum.reshape(colors, rows, group_sites)
        own = group * (pieces // groups)
        for c in range(colors):
            for k in range(pieces // groups):
                outgoing[c * pieces + own + k] = spectrum[c, :, k * width : (k + 1) * width]

        def start_out(offset, carry):
            to = lax.rem(me + offset, parts)
            kind = lax.rem(to, pieces)

            @pl.when(jnp.logical_and(kind >= own, kind < own + pieces // groups))
            def _():
                out_copy(to, me).start()

            return carry

        lax.fori_loop(1, parts, start_out, 0)

    def wait_out(offset, carry):
        other = lax.rem(me + offset, parts)
        out_copy(other, other).wait()
        return carry

    gathered[own_rows(me), :] = outgoing[me]
    lax.fori_loop(1, parts, wait_out, 0)

    def mix(source, target, weighted):
        total_rows = mix_xy.shape[0]
        size = min(total_rows, LANES)

        def block(index, carry):
            at = pl.ds(pl.multiple_of(index * size, size), size)
            mixed = jnp.dot(
                mix_xy[at, :], source[...], preferred_element_type=jnp.float32,
                precision=lax.Precision.HIGHEST,
            )
            target[at, :] = mixed * weights[at, :] if weighted else mixed
            return carry

        lax.fori_loop(0, total_rows // size, block, 0)

    mix(gathered, filtered, True)
    mix(filtered, gathered, False)

    def back_copy(to, source):
        return pltpu.make_async_remote_copy(
            gathered.at[own_rows(to)], returned.at[source], back_send.at[to], back_recv.at[source],
            device_id=place(to),
        )

    def start_back(offset, carry):
        back_copy(lax.rem(me + offset, parts), me).start()
        return carry

    def wait_back(offset, carry):
        other = lax.rem(me + offset, parts)
        back_copy(other, other).wait()
        return carry

    lax.fori_loop(1, parts, start_back, 0)
    returned[me] = gathered[own_rows(me), :]
    lax.fori_loop(1, parts, wait_back, 0)

    back = jnp.concatenate(
        [
            jnp.concatenate([returned[c * pieces + k] for k in range(pieces)], axis=1)
            for c in range(colors)
        ],
        axis=0,
    )
    total[...] = plane_transform(back, table_high, table_low).reshape(colors, rows, sites)

    def update(j, carry):
        lanes = pl.ds(pl.multiple_of(j * LANES, LANES), LANES)
        rotation = rotation_rows([total[a, :, lanes] for a in range(8)])
        updated = product(rotation, load_link(links.at[0], lanes))
        for r in range(2):
            for k in range(3):
                out_link[3 * r + k, :, lanes] = updated[r][k][0]
                out_link[6 + 3 * r + k, :, lanes] = updated[r][k][1]
        return carry

    lax.fori_loop(0, chunks, update, 0)


def shards(gauge_links, momentum):
    gx_count, gy_count = lax.axis_size("gx"), lax.axis_size("gy")
    colors, layers, rows, sites = momentum.shape
    assert layers == 1
    parts = gx_count * gy_count
    width = colors * sites // parts
    assert sites % width == 0
    links = gauge_links.reshape(4, 12, rows, sites)
    fields = momentum.reshape(colors, rows, sites)
    f32 = jnp.float32
    everything = rows * parts
    dma = pltpu.SemaphoreType.DMA

    def body(*refs):
        step_kernel(gx_count, gy_count, *refs)

    constants = tables(gx_count * layers, gy_count * rows, colors, parts)
    grant = 67043328 - 3000 * 1024
    vmem = pl.BlockSpec(memory_space=pltpu.VMEM)
    new_momentum, new_link = pl.pallas_call(
        body,
        out_shape=(
            jax.ShapeDtypeStruct((colors, rows, sites), f32),
            jax.ShapeDtypeStruct((12, rows, sites), f32),
        ),
        in_specs=[pl.BlockSpec(memory_space=pltpu.HBM)] + [vmem] * 6,
        out_specs=(vmem, vmem),
        scratch_shapes=[
            pltpu.VMEM((4, 12, rows, sites), f32),
            pltpu.VMEM((3, 18, rows, sites), f32),
            pltpu.VMEM((3, 10, rows, sites), f32),
            pltpu.VMEM((3, 10, rows, sites), f32),
            pltpu.VMEM((12, rows, sites), f32),
            pltpu.VMEM((3, 12, rows, sites), f32),
            pltpu.VMEM((3, colors, rows, sites), f32),
            pltpu.VMEM((colors, rows, sites), f32),
            pltpu.VMEM((colors, rows, sites), f32),
            pltpu.VMEM((parts, rows, width), f32),
            pltpu.VMEM((everything, width), f32),
            pltpu.VMEM((everything, width), f32),
            pltpu.VMEM((parts, rows, width), f32),
            pltpu.VMEM((sites, sites), jnp.bfloat16),
            pltpu.VMEM((sites, sites), jnp.bfloat16),
            pltpu.VMEM((everything, width), f32),
            dma((4,)), dma((3 * HALVES,)), dma((3 * HALVES,)), dma((2,)), dma((2,)),
            dma((parts,)), dma((parts,)), dma((parts,)), dma((parts,)),
        ],
        compiler_params=pltpu.CompilerParams(
            collective_id=0, has_side_effects=True, vmem_limit_bytes=grant
        ),
    )(links, fields, *constants)
    return (new_momentum.reshape(momentum.shape), new_link.reshape((12,) + momentum.shape[1:]))


def solution(mesh):
    return jax.shard_map(
        shards,
        mesh=mesh,
        in_specs=(P(None, None, ("cfg", "gx"), "gy", None), P(None, ("cfg", "gx"), "gy", None)),
        out_specs=(P(None, ("cfg", "gx"), "gy", None), P(None, ("cfg", "gx"), "gy", None)),
        check_vma=False,
    )
```
